32 devices in a mesh: blk: 32 (over z, y, x, core).
Axes of the slice: x: 2, y: 2, z: 4, core: 2. Of those that a mesh axis runs over, the one named last changes fastest.
Arguments:
- defect: float32 [384, 128], P('blk'), may hold values from -6 to 6
- mass: float32 [384, 128], P('blk'), may hold values from 1 to 2
- block_diag: float32 [384, 128, 128], P('blk'), may hold values from -0.1875 to 0.1875
- coupling: float32 [3072, 128, 128], P('blk'), may hold values from -0.09375 to 0.09375
- tile_rows: int32 [3072], P('blk'), may hold values from 0 to 383, as said below
- tile_cols: int32 [3072], P('blk'), may hold values from 0 to 383, as said below
Outputs:
- update: float32 [384, 128], P('blk')
The draws below stay inside these ranges and needn't reach their ends.
Inputs may be any that keep to these rules, and one draw needn't show every extreme that they name: `tile_rows`: block rows d * 12 to d * 12 + 11 belong to device d of blk, and each device holds the tiles at positions d * 96 to d * 96 + 95. Of every tile a device holds, exactly one of its block row and block column belongs to that device; the other belongs to a different device. Exactly half of the 96 tiles of every device have their block row with that device, and the other half their block column. A program may send only the blocks and products of tiles that exist; slots of a padded buffer that no tile fills need not be sent. `tile_cols`: of one device's tiles, at most 2 have their block column with any one other device and at most 2 have their block row with any one other device; every device reaches 2 with some other device on each of the two sides.
All inputs are finite; a program needn't handle non-finite values.
Results may differ from the reference program's by a relative error of at most 0.0001.
Values sent between devices are 32-bit elements; how exact they have to be, the bound alone decides.
A program may use at most 64 MiB of HBM per device.

```python
import jax
import jax.numpy as jnp
from jax import lax

B = 128
K = 8
RB = 12
ITERS = 3
TD = 96
C = 2
NB = 384
NT = 3072
N_BLK = 32


def tile_pattern(key):
    base = jax.random.fold_in(key, 11)
    half = TD // 2
    peers = N_BLK - 1
    cells = peers * C
    antipode_lane = N_BLK // 2 - 1

    def one_device(device_key, device):
        keys = jax.random.split(device_key, 6)

        def pick(pick_key):
            order = jax.random.permutation(pick_key, cells).astype(jnp.int32)
            grid = jnp.arange(cells, dtype=jnp.int32)
            score = jnp.where(grid // C == antipode_lane, grid - cells, order)
            return (jnp.argsort(score, stable=True)[:half] // C).astype(jnp.int32)
        lanes = jnp.concatenate([pick(keys[1]), pick(keys[2])])
        far_device = (device + lanes + 1) % N_BLK
        own_slot = jax.random.randint(keys[3], (TD,), 0, RB).astype(jnp.int32)
        far_slot = jax.random.randint(keys[4], (TD,), 0, RB).astype(jnp.int32)
        own_block = device * RB + own_slot
        far_block = far_device * RB + far_slot
        first = jnp.arange(TD) < half
        rows = jnp.where(first, own_block, far_block)
        cols = jnp.where(first, far_block, own_block)
        shuffle = jax.random.permutation(keys[5], TD)
        return (rows[shuffle], cols[shuffle])
    owners = jnp.arange(N_BLK, dtype=jnp.int32)
    rows, cols = jax.vmap(one_device)(jax.random.split(base, N_BLK), owners)
    return (rows.reshape(NT).astype(jnp.int32), cols.reshape(NT).astype(jnp.int32))


def draw_tile_rows(key, part):
    return tile_pattern(key)[0]


def draw_tile_cols(key, part):
    return tile_pattern(key)[1]


def levels(rng, dims, cuts, least, top_value):
    def one(axis_at, blocks):
        steps = jax.random.uniform(jax.random.fold_in(jax.random.fold_in(rng, 6), axis_at), (blocks,), jnp.float32, least / len(cuts), top_value / len(cuts))
        return jnp.repeat(jnp.exp(steps), dims[axis_at] // blocks).reshape((-1,) + (1,) * (len(dims) - axis_at - 1))

    loudness = one(*cuts[0])
    for cut in cuts[1:]:
        loudness = loudness * one(*cut)
    return loudness


def gaussian(key, shape, scale, limit, cuts=(), held_as=jnp.bfloat16):
    drawn = jax.random.normal(key, shape, jnp.float32) * scale
    if len(cuts) > 0:
        drawn = levels(key, shape, cuts, -0.22, 0.18) * drawn
    return jnp.clip(drawn, min=-limit, max=limit).astype(held_as)


def setup_inputs(seed: int = 0) -> dict:
    splits = jax.random.split(jax.random.key(seed), 7)
    return {
        "defect": gaussian(splits[0], (NB, B), 1.0, 6.0, ((0, 32),), jnp.float32),
        "mass": jnp.clip(1.0 + 1.0 * jax.random.uniform(splits[1], (NB, B), jnp.float32) ** levels(splits[1], (NB, B), ((0, 32),), -0.2, 0.2), 1.0, 2.0),
        "block_diag": gaussian(splits[2], (NB, B, B), (8 * B) ** -0.5, 0.1875, ((0, 32),), jnp.float32),
        "coupling": gaussian(splits[3], (NT, B, B), (4 * K * B) ** -0.5, 0.09375, ((0, 32),), jnp.float32),
        "tile_rows": draw_tile_rows(jax.random.fold_in(splits[6], 71), 0),
        "tile_cols": draw_tile_cols(jax.random.fold_in(splits[6], 71), 0),
    }


def solve_small(gram, target):
    factor = jnp.linalg.cholesky(gram)
    count = gram.shape[0]
    forward = []
    for index in range(count):
        value = target[index]
        for inner in range(index):
            value = value - factor[index, inner] * forward[inner]
        forward.append(value / factor[index, index])
    backward = [None] * count
    for index in reversed(range(count)):
        value = forward[index]
        for inner in range(index + 1, count):
            value = value - factor[inner, index] * backward[inner]
        backward[index] = value / factor[index, index]
    return backward

def newton_apply(vector, mass, block_diag, coupling, tile_rows, tile_cols):
    own = jnp.einsum('rij,rj->ri', block_diag, vector, precision=lax.Precision.HIGHEST)
    products = jnp.einsum('tij,tj->ti', coupling, vector[tile_cols], precision=lax.Precision.HIGHEST)
    far = jax.ops.segment_sum(products, tile_rows, num_segments=NB)
    return mass * vector + own + far

def reference(defect, mass, block_diag, coupling, tile_rows, tile_cols):
    negated = -defect
    beta = jnp.sqrt(jnp.sum(negated * negated))
    basis = [negated / beta]
    upper = jnp.zeros((ITERS + 1, ITERS), jnp.float32)
    for column in range(ITERS):
        image = newton_apply(basis[column], mass, block_diag, coupling, tile_rows, tile_cols)
        dots = jnp.stack([jnp.sum(item * image) for item in basis])
        for index in range(column + 1):
            image = image - dots[index] * basis[index]
        norm = jnp.sqrt(jnp.sum(image * image))
        upper = upper.at[:column + 1, column].set(dots)
        upper = upper.at[column + 1, column].set(norm)
        if column + 1 < ITERS:
            basis.append(image / norm)
    gram = jnp.dot(upper.T.astype(jnp.float32), upper.astype(jnp.float32), precision=lax.Precision.HIGHEST, preferred_element_type=jnp.float32)
    mixing = solve_small(gram, beta * upper[0, :])
    update = jnp.zeros_like(defect)
    for index in range(ITERS):
        update = update + mixing[index] * basis[index]
    return update
```

```python
import functools

import jax
import jax.numpy as jnp
from jax import lax
from jax.experimental import pallas as pl
from jax.experimental.pallas import tpu as pltpu
from jax.sharding import PartitionSpec as P

ITERS = 3
F32 = jnp.float32
MESH = pl.DeviceIdType.MESH
STEP = 12


def iota(shape, axis):
    return lax.broadcasted_iota(jnp.int32, shape, axis)


def iota_f(shape, axis):
    return iota(shape, axis).astype(F32)


def dot(a, b):
    return lax.dot_general(
        a,
        b,
        (((1,), (0,)), ((), ())),
        precision=lax.Precision.HIGHEST,
        preferred_element_type=F32,
    )


def total(value):
    return jnp.sum(jnp.sum(value, axis=0, keepdims=True), axis=1, keepdims=True)


def as_row(items):
    lane = iota((1, 128), 1)
    row = jnp.zeros((1, 128), F32)
    for index, item in enumerate(items):
        row = jnp.where(lane == index, item, row)
    return row


def pick(row, index):
    lane = iota((1, 128), 1)
    return jnp.sum(jnp.where(lane == index, row, 0.0), axis=1, keepdims=True)


def kernel(
    n,
    slots,
    defect_ref,
    mass_ref,
    diag_hbm,
    coup_hbm,
    rows_ref,
    cols_ref,
    out_ref,
    coup,
    diag,
    order_v,
    order_s,
    mass16,
    wbuf,
    xbuf,
    ask_hot,
    land_hot,
    send0,
    recv0,
    send_a,
    recv_a,
    send_b,
    recv_b,
    send_f,
    recv_f,
    load_sems,
    order_sem,
    sent,
    got,
):
    me = lax.axis_index("blk")
    rb, width = defect_ref.shape
    tiles = rows_ref.shape[1]
    half = tiles // 2
    pad = wbuf.shape[0]
    head = send0.shape[0]
    parts = 4
    chunk = tiles // parts

    loads = [pltpu.make_async_copy(diag_hbm, diag, load_sems.at[parts])]
    for part in range(parts):
        span = pl.ds(part * chunk, chunk)
        loads.append(
            pltpu.make_async_copy(coup_hbm.at[span], coup.at[span], load_sems.at[part])
        )
    for item in loads:
        item.start()

    barrier = pltpu.get_barrier_semaphore()

    def greet(k, carry):
        pl.semaphore_signal(
            barrier, inc=1, device_id=(lax.rem(me + k, n),), device_id_type=MESH
        )
        return carry

    lax.fori_loop(1, n, greet, 0)

    rows = rows_ref[...]
    cols = cols_ref[...]
    low = me * rb
    pushes = (rows < low) | (rows >= low + rb)
    push_l = jnp.where(pushes, 1.0, 0.0)
    rem_l = jnp.where(pushes, rows, cols).astype(F32)
    loc_l = (jnp.where(pushes, cols, rows) - low).astype(F32)
    own_l = jnp.floor((rem_l + 0.5) * (1.0 / rb))
    far_l = rem_l - own_l * rb
    me_f = me.astype(F32)
    rel_l = own_l - me_f - 1.0
    rel_l = jnp.where(rel_l < 0.0, rel_l + n, rel_l)
    key_l = own_l + push_l * n
    square = (tiles, tiles)
    eye = iota(square, 0) == iota(square, 1)

    def to_s(value):
        return jnp.sum(jnp.where(eye, value, 0.0), axis=1, keepdims=True)

    earlier = iota(square, 0) < iota(square, 1)
    key_s = to_s(key_l)
    push_s = to_s(push_l)
    slot_l = jnp.sum(
        jnp.where((key_s == key_l) & earlier, 1.0, 0.0), axis=0, keepdims=True
    )
    pos_l = jnp.sum(
        jnp.where((push_s < push_l) | ((push_s == push_l) & earlier), 1.0, 0.0),
        axis=0,
        keepdims=True,
    )
    pos_s = to_s(pos_l)
    slot_s = to_s(slot_l)
    own_s = to_s(own_l)
    far_s = to_s(far_l)
    loc_s = to_s(loc_l)
    u_l = rel_l * 8.0 + slot_l
    u_s = to_s(u_l)
    wide = (tiles, 128)
    lane_w = iota_f(wide, 1)
    push_int = jnp.where(pushes, 1, 0)
    push_down = jnp.sum(jnp.where(eye, push_int, 0), axis=1, keepdims=True)
    place = jnp.sum(
        jnp.where(
            (push_down < push_int) | ((push_down == push_int) & earlier), 1, 0
        ),
        axis=0,
        keepdims=True,
    )
    place_down = jnp.sum(jnp.where(eye, place, 0), axis=1, keepdims=True)
    order_v[...] = jnp.sum(
        jnp.where(place_down == iota(wide, 1), iota(wide, 0), 0), axis=0, keepdims=True
    )
    order_copy = pltpu.make_async_copy(order_v, order_s, order_sem)
    order_copy.start()
    lane_1 = iota_f((1, 128), 1)
    push_u = jnp.sum(jnp.where(pos_s == lane_w + half, u_s, 0.0), axis=0, keepdims=True)
    push_u = jnp.where(lane_1 < half, push_u, -1.0)
    fetch_row = jnp.sum(jnp.where(pos_s == lane_w, loc_s, 0.0), axis=0, keepdims=True)
    fetch_row = jnp.where(lane_1 < half, fetch_row, -1.0)
    sorted_shape = (half, tiles)
    fetch_here = pos_l == iota_f(sorted_shape, 0)
    push_here = pos_l == iota_f(sorted_shape, 0) + half
    fetch_u = jnp.sum(jnp.where(fetch_here, u_l, 0.0), axis=1, keepdims=True)
    fetch_v = jnp.sum(
        jnp.where(fetch_here, rel_l * head + far_l, 0.0), axis=1, keepdims=True
    )
    push_col = jnp.sum(jnp.where(push_here, loc_l, 0.0), axis=1, keepdims=True)
    lane_key = own_s * slots + slot_s
    asks = jnp.sum(
        jnp.where((lane_key == lane_w) & (push_s < 0.5), far_s + 1.0, 0.0),
        axis=0,
        keepdims=True,
    ) - 1.0
    goals = jnp.sum(
        jnp.where((lane_key == lane_w) & (push_s > 0.5), far_s + 1.0, 0.0),
        axis=0,
        keepdims=True,
    ) - 1.0
    slots8 = n * 8

    def hot(mask):
        return jnp.where(mask, 1.0, 0.0)

    wbuf[...] = jnp.zeros(wbuf.shape, F32)
    wbuf[0:rb, :] = -defect_ref[...]
    mass16[...] = jnp.zeros(mass16.shape, F32)
    mass16[0:rb, :] = mass_ref[...]
    vector = wbuf[...]
    send0[...] = jnp.zeros(send0.shape, F32)
    send0[0:rb, :] = -defect_ref[...]
    own_part = as_row([total(vector * vector)])
    send0[rb : rb + 1, :] = own_part
    send0[rb + 1 : rb + 2, :] = asks
    send0[rb + 2 : rb + 3, :] = goals
    recv0[n - 1] = jnp.zeros(recv0.shape[1:], F32)
    for turn in range(ITERS):
        recv_b[turn, n - 1] = jnp.zeros((8, 128), F32)
    for turn in range(ITERS - 1):
        recv_a[turn, n - 1] = jnp.zeros((8, 128), F32)
    recv_f[n - 1] = jnp.zeros((8, 128), F32)

    pl.semaphore_wait(barrier, n - 1)

    def broadcast(source, target, index, spread):
        def one(k, carry):
            pltpu.make_async_remote_copy(
                src_ref=source.at[k - 1] if spread else source,
                dst_ref=target.at[n - 1 - k],
                send_sem=sent.at[index],
                recv_sem=got.at[index],
                device_id=(lax.rem(me + k, n),),
                device_id_type=MESH,
            ).start()
            return carry

        lax.fori_loop(1, n, one, 0)

    def await_all(target, sem):
        view = target.at[pl.ds(0, n - 1)]
        pltpu.make_async_copy(view, view, sem).wait()

    broadcast(send0, recv0, 0, False)

    spread_hot = hot(iota_f((slots8, 128), 0) == push_u)
    fetch_hot = hot(iota_f((half, slots8), 1) == fetch_u)
    first_hot = hot(iota_f((half, n * head), 1) == fetch_v)
    input_hot = hot(iota_f((half, pad), 1) == push_col)
    kept_hot = hot(iota_f((pad, 128), 0) == fetch_row)

    lane_k = iota((width, 128), 1)

    def matvec(acc, tile, index):
        row = xbuf[pl.ds(index, 1), :]
        value = jnp.sum(tile * row, axis=1, keepdims=True)
        return jnp.where(lane_k == index, value, acc)

    def coupled(base, acc):
        def body(step, acc):
            for inner in range(STEP):
                index = step * STEP + inner
                tile = jnp.clip(order_s[0, base + index], 0, 2 * half - 1)
                acc = matvec(acc, coup[tile], index)
            return acc

        return lax.fori_loop(0, half // STEP, body, acc)

    empty = jnp.zeros((width, 128), F32)

    def begin(turn, vector):
        xbuf[0:half, :] = dot(input_hot, vector)
        xbuf[half : half + pad, :] = vector
        acc = empty
        for index in range(rb):
            acc = matvec(acc, diag[index], half + index)
        acc = coupled(half, acc)
        found = acc.T
        send_b[turn] = dot(spread_hot, found).reshape(n, 8, 128)
        broadcast(send_b.at[turn], recv_b.at[turn], 1 + 2 * turn, True)
        return mass16[...] * vector + found[half : half + pad, :]

    def finish(turn, image, inputs):
        xbuf[0:half, :] = inputs
        found = coupled(0, empty).T
        image = image + dot(kept_hot, found)
        await_all(recv_b.at[turn], got.at[1 + 2 * turn])
        arrived = recv_b[turn].reshape(slots8, 128)
        return image + dot(land_hot[...], arrived)

    for item in loads:
        item.wait()
    order_copy.wait()

    image = begin(0, vector)
    await_all(recv0, got.at[0])
    lane_3 = iota((n, 8, 128), 2)
    sub_3 = iota((n, 8, 128), 1)
    peer_3 = iota((n, 8, 128), 0)
    mine = (lane_3 == me * slots + sub_3) & (sub_3 < slots) & (peer_3 < n - 1)

    def addressed(offset):
        line = recv0[:, rb + offset : rb + offset + 1, :]
        line = jnp.broadcast_to(line, (n, 8, 128))
        found = jnp.sum(jnp.where(mine, line + 1.0, 0.0), axis=2, keepdims=True) - 1.0
        return hot(found == lane_3.astype(F32)).reshape(slots8, 128)

    land_hot[...] = addressed(2).T[0:pad, :]
    ask_hot[...] = addressed(1)
    squares = jnp.sum(recv0[:, rb, :], axis=0, keepdims=True) + own_part
    beta = jnp.sqrt(pick(squares, 0))
    inputs = dot(first_hot, recv0[...].reshape(n * head, 128))
    image = finish(0, image, inputs)
    basis = [vector / beta]
    images = [image / beta]
    heads = []
    gram = {}

    for turn in range(1, ITERS):
        vector = images[-1]
        own_part = as_row(
            [total(vector * item) for item in basis]
            + [total(vector * item) for item in images]
        )
        wide_vector = jnp.concatenate([vector, jnp.zeros((128 - pad, 128), F32)], axis=0)
        blocks = dot(ask_hot[...], wide_vector).reshape(n, 8, 128)
        sub = iota((n, 8, 128), 1)
        blocks = jnp.where(sub == slots, own_part.reshape(1, 1, 128), blocks)
        send_a[turn - 1] = blocks
        broadcast(send_a.at[turn - 1], recv_a.at[turn - 1], 2 * turn, True)
        image = begin(turn, vector)
        await_all(recv_a.at[turn - 1], got.at[2 * turn])
        sums = jnp.sum(recv_a[turn - 1][:, slots, :], axis=0, keepdims=True) + own_part
        inputs = dot(fetch_hot, recv_a[turn - 1].reshape(slots8, 128))
        image = finish(turn, image, inputs)
        dots = [pick(sums, index) for index in range(turn)]
        for index in range(turn):
            gram[index, turn - 1] = pick(sums, turn + index)
        heads.append(dots[0])
        square = gram[turn - 1, turn - 1]
        left = square
        for value in dots:
            left = left - value * value
        scale = lax.rsqrt(jnp.maximum(left, square * 1e-6))
        for index in range(turn):
            vector = vector - dots[index] * basis[index]
            image = image - dots[index] * images[index]
        basis.append(vector * scale)
        images.append(image * scale)

    vector = images[-1]
    own_part = as_row(
        [total(vector * basis[0])] + [total(vector * item) for item in images]
    )
    send_f[...] = jnp.broadcast_to(own_part, (8, 128))
    broadcast(send_f, recv_f, 2 * ITERS, False)
    await_all(recv_f, got.at[2 * ITERS])
    sums = jnp.sum(recv_f[:, 0, :], axis=0, keepdims=True) + own_part
    heads.append(pick(sums, 0))
    for index in range(ITERS):
        gram[index, ITERS - 1] = pick(sums, 1 + index)

    factor = {}
    for i in range(ITERS):
        for j in range(i + 1):
            value = gram[j, i]
            for k in range(j):
                value = value - factor[i, k] * factor[j, k]
            factor[i, j] = jnp.sqrt(value) if i == j else value / factor[j, j]
    forward = []
    for i in range(ITERS):
        value = beta * heads[i]
        for k in range(i):
            value = value - factor[i, k] * forward[k]
        forward.append(value / factor[i, i])
    mixing = [None] * ITERS
    for i in reversed(range(ITERS)):
        value = forward[i]
        for k in range(i + 1, ITERS):
            value = value - factor[k, i] * mixing[k]
        mixing[i] = value / factor[i, i]
    update = mixing[0] * basis[0]
    for i in range(1, ITERS):
        update = update + mixing[i] * basis[i]
    out_ref[...] = update[0:rb, :]

    await_all(recv0, sent.at[0])
    for turn in range(ITERS):
        await_all(send_b.at[turn], sent.at[1 + 2 * turn])
    for turn in range(1, ITERS):
        await_all(send_a.at[turn - 1], sent.at[2 * turn])
    await_all(recv_f, sent.at[2 * ITERS])


def on_device(defect, mass, block_diag, coupling, tile_rows, tile_cols):
    rb, width = defect.shape
    tiles = tile_rows.shape[0]
    n = lax.axis_size("blk")
    slots = (tiles // 2 + n - 2) // (n - 1)
    pad = -(-rb // 8) * 8
    head = -(-(rb + 3) // 8) * 8
    vmem = pl.BlockSpec(memory_space=pltpu.VMEM)
    hbm = pl.BlockSpec(memory_space=pl.ANY)
    return pl.pallas_call(
        functools.partial(kernel, n, slots),
        out_shape=jax.ShapeDtypeStruct((rb, width), F32),
        in_specs=[vmem, vmem, hbm, hbm, vmem, vmem],
        out_specs=vmem,
        scratch_shapes=[
            pltpu.VMEM((tiles, width, width), F32),
            pltpu.VMEM((rb, width, width), F32),
            pltpu.VMEM((1, 128), jnp.int32),
            pltpu.SMEM((1, 128), jnp.int32),
            pltpu.VMEM((pad, width), F32),
            pltpu.VMEM((pad, width), F32),
            pltpu.VMEM((tiles, width), F32),
            pltpu.VMEM((n * 8, 128), F32),
            pltpu.VMEM((pad, n * 8), F32),
            pltpu.VMEM((head, width), F32),
            pltpu.VMEM((n, head, width), F32),
            pltpu.VMEM((ITERS - 1, n, 8, width), F32),
            pltpu.VMEM((ITERS - 1, n, 8, width), F32),
            pltpu.VMEM((ITERS, n, 8, width), F32),
            pltpu.VMEM((ITERS, n, 8, width), F32),
            pltpu.VMEM((8, width), F32),
            pltpu.VMEM((n, 8, width), F32),
            pltpu.SemaphoreType.DMA((5,)),
            pltpu.SemaphoreType.DMA,
            pltpu.SemaphoreType.DMA((2 * ITERS + 1,)),
            pltpu.SemaphoreType.DMA((2 * ITERS + 1,)),
        ],
        compiler_params=pltpu.CompilerParams(collective_id=0, has_side_effects=True),
    )(
        defect,
        mass,
        block_diag,
        coupling,
        tile_rows.reshape(1, tiles),
        tile_cols.reshape(1, tiles),
    )


def solution(mesh):
    in_specs = (
        P("blk", None),
        P("blk", None),
        P("blk", None, None),
        P("blk", None, None),
        P("blk"),
        P("blk"),
    )
    return jax.shard_map(
        on_device, mesh=mesh, in_specs=in_specs, out_specs=P("blk", None), check_vma=False
    )
```

```python
import functools

import jax
import jax.numpy as jnp
from jax import lax
from jax.experimental import pallas as pl
from jax.experimental.pallas import tpu as pltpu
from jax.sharding import PartitionSpec as P

ITERS = 3
F32 = jnp.float32
MESH = pl.DeviceIdType.MESH
STEP = 16


def iota(shape, axis):
    return lax.broadcasted_iota(jnp.int32, shape, axis)


def iota_f(shape, axis):
    return iota(shape, axis).astype(F32)


def dot(hot, value):
    hot = hot.astype(jnp.bfloat16)
    out = None
    for _ in range(3):
        piece = value.astype(jnp.bfloat16)
        value = value - piece.astype(F32)
        term = lax.dot_general(
            hot, piece, (((1,), (0,)), ((), ())), preferred_element_type=F32
        )
        out = term if out is None else out + term
    return out


def total(value):
    return jnp.sum(jnp.sum(value, axis=0, keepdims=True), axis=1, keepdims=True)


def as_row(items):
    lane = iota((1, 128), 1)
    row = jnp.zeros((1, 128), F32)
    for index, item in enumerate(items):
        row = jnp.where(lane == index, item, row)
    return row


def pick(row, index):
    lane = iota((1, 128), 1)
    return jnp.sum(jnp.where(lane == index, row, 0.0), axis=1, keepdims=True)


def kernel(
    n,
    slots,
    defect_ref,
    mass_ref,
    diag_hbm,
    coup_hbm,
    rows_ref,
    cols_ref,
    out_ref,
    coup,
    diag,
    order_v,
    order_s,
    mass16,
    wbuf,
    xbuf,
    ask_hot,
    land_hot,
    send0,
    recv0,
    send_a,
    recv_a,
    send_b,
    recv_b,
    send_f,
    recv_f,
    load_sems,
    order_sem,
    sent,
    got,
):
    me = lax.axis_index("blk")
    rb, width = defect_ref.shape
    tiles = rows_ref.shape[1]
    half = tiles // 2
    pad = wbuf.shape[0]
    head = send0.shape[1]
    parts = 4
    chunk = tiles // parts

    loads = [pltpu.make_async_copy(diag_hbm, diag, load_sems.at[parts])]
    for part in range(parts):
        span = pl.ds(part * chunk, chunk)
        loads.append(
            pltpu.make_async_copy(coup_hbm.at[span], coup.at[span], load_sems.at[part])
        )
    for item in loads:
        item.start()

    barrier = pltpu.get_barrier_semaphore()

    def peer(k):
        there = me + k
        return jnp.where(there >= n, there - n, there)

    for k in range(1, n):
        pl.semaphore_signal(barrier, inc=1, device_id=(peer(k),), device_id_type=MESH)

    rows = rows_ref[...]
    cols = cols_ref[...]
    low = me * rb
    pushes = (rows < low) | (rows >= low + rb)
    push_l = jnp.where(pushes, 1.0, 0.0)
    rem_l = jnp.where(pushes, rows, cols).astype(F32)
    loc_l = (jnp.where(pushes, cols, rows) - low).astype(F32)
    own_l = jnp.floor((rem_l + 0.5) * (1.0 / rb))
    far_l = rem_l - own_l * rb
    me_f = me.astype(F32)
    rel_l = own_l - me_f - 1.0
    rel_l = jnp.where(rel_l < 0.0, rel_l + n, rel_l)
    key_l = own_l + push_l * n
    square = (tiles, tiles)
    eye = iota(square, 0) == iota(square, 1)

    def to_s(value):
        return jnp.sum(jnp.where(eye, value, 0.0), axis=1, keepdims=True)

    earlier = iota(square, 0) < iota(square, 1)
    key_s = to_s(key_l)
    push_s = to_s(push_l)
    slot_l = jnp.sum(
        jnp.where((key_s == key_l) & earlier, 1.0, 0.0), axis=0, keepdims=True
    )
    pos_l = jnp.sum(
        jnp.where((push_s < push_l) | ((push_s == push_l) & earlier), 1.0, 0.0),
        axis=0,
        keepdims=True,
    )
    pos_s = to_s(pos_l)
    slot_s = to_s(slot_l)
    own_s = to_s(own_l)
    far_s = to_s(far_l)
    loc_s = to_s(loc_l)
    lines = slots + 1
    u_l = rel_l * lines + slot_l
    u_s = to_s(rel_l * slots + slot_l)
    wide = (tiles, 128)
    lane_w = iota_f(wide, 1)
    push_int = jnp.where(pushes, 1, 0)
    push_down = jnp.sum(jnp.where(eye, push_int, 0), axis=1, keepdims=True)
    place = jnp.sum(
        jnp.where(
            (push_down < push_int) | ((push_down == push_int) & earlier), 1, 0
        ),
        axis=0,
        keepdims=True,
    )
    place_down = jnp.sum(jnp.where(eye, place, 0), axis=1, keepdims=True)
    order_v[...] = jnp.sum(
        jnp.where(place_down == iota(wide, 1), iota(wide, 0), 0), axis=0, keepdims=True
    )
    order_copy = pltpu.make_async_copy(order_v, order_s, order_sem)
    order_copy.start()
    lane_1 = iota_f((1, 128), 1)
    push_u = jnp.sum(jnp.where(pos_s == lane_w + half, u_s, 0.0), axis=0, keepdims=True)
    push_u = jnp.where(lane_1 < half, push_u, -1.0)
    fetch_row = jnp.sum(jnp.where(pos_s == lane_w, loc_s, 0.0), axis=0, keepdims=True)
    fetch_row = jnp.where(lane_1 < half, fetch_row, -1.0)
    sorted_shape = (half, tiles)
    fetch_here = pos_l == iota_f(sorted_shape, 0)
    push_here = pos_l == iota_f(sorted_shape, 0) + half
    fetch_u = jnp.sum(jnp.where(fetch_here, u_l, 0.0), axis=1, keepdims=True)
    fetch_v = jnp.sum(
        jnp.where(fetch_here, rel_l * head + far_l, 0.0), axis=1, keepdims=True
    )
    push_col = jnp.sum(jnp.where(push_here, loc_l, 0.0), axis=1, keepdims=True)
    lane_key = own_s * slots + slot_s
    asks = jnp.sum(
        jnp.where((lane_key == lane_w) & (push_s < 0.5), far_s + 1.0, 0.0),
        axis=0,
        keepdims=True,
    ) - 1.0
    goals = jnp.sum(
        jnp.where((lane_key == lane_w) & (push_s > 0.5), far_s + 1.0, 0.0),
        axis=0,
        keepdims=True,
    ) - 1.0
    lines_all = n * lines
    slots_all = n * slots

    def hot(mask):
        return jnp.where(mask, 1.0, 0.0)

    wbuf[...] = jnp.zeros(wbuf.shape, F32)
    wbuf[0:rb, :] = -defect_ref[...]
    mass16[...] = jnp.zeros(mass16.shape, F32)
    mass16[0:rb, :] = mass_ref[...]
    vector = wbuf[...]
    send0[...] = jnp.zeros(send0.shape, F32)
    send0[0, 0:rb, :] = -defect_ref[...]
    own_part = as_row([total(vector * vector)])
    send0[0, rb : rb + 1, :] = own_part
    send0[0, rb + 1 : rb + 2, :] = asks
    send0[0, rb + 2 : rb + 3, :] = goals
    recv0[n - 1] = jnp.zeros(recv0.shape[1:], F32)
    for turn in range(ITERS):
        recv_b[turn, slots_all - slots : slots_all] = jnp.zeros((slots, 1, 128), F32)
    for turn in range(ITERS - 1):
        recv_a[turn, lines_all - lines : lines_all] = jnp.zeros((lines, 1, 128), F32)
    recv_f[n - 1] = jnp.zeros((1, 128), F32)

    pl.semaphore_wait(barrier, n - 1)

    def broadcast(source, target, index, count, spread):
        for k in range(1, n):
            start = (n - 1 - k) * count
            pltpu.make_async_remote_copy(
                src_ref=source.at[pl.ds((k - 1) * count, count)] if spread else source,
                dst_ref=target.at[pl.ds(start, count)],
                send_sem=sent.at[index],
                recv_sem=got.at[index],
                device_id=(peer(k),),
                device_id_type=MESH,
            ).start()

    def await_all(target, sem, count):
        view = target.at[pl.ds(0, (n - 1) * count)]
        pltpu.make_async_copy(view, view, sem).wait()

    broadcast(send0, recv0, 0, 1, False)

    spread_hot = hot(iota_f((slots_all, 128), 0) == push_u)
    fetch_hot = hot(iota_f((half, lines_all), 1) == fetch_u)
    first_hot = hot(iota_f((half, n * head), 1) == fetch_v)
    input_hot = hot(iota_f((half, pad), 1) == push_col)
    kept_hot = hot(iota_f((pad, 128), 0) == fetch_row)

    lane_k = iota((width, 128), 1)

    def matvec(acc, tile, index):
        row = xbuf[pl.ds(index, 1), :]
        value = jnp.sum(tile * row, axis=1, keepdims=True)
        return jnp.where(lane_k == index, value, acc)

    def coupled(base, acc):
        def body(step, acc):
            for inner in range(STEP):
                index = step * STEP + inner
                tile = jnp.clip(order_s[0, base + index], 0, 2 * half - 1)
                acc = matvec(acc, coup[tile], index)
            return acc

        return lax.fori_loop(0, half // STEP, body, acc)

    empty = jnp.zeros((width, 128), F32)

    def begin(turn, vector):
        xbuf[0:half, :] = dot(input_hot, vector)
        found = coupled(half, empty).T
        send_b[turn, :, 0, :] = dot(spread_hot, found)
        broadcast(send_b.at[turn], recv_b.at[turn], 1 + 2 * turn, slots, True)
        wbuf[...] = vector
        acc = empty
        for index in range(rb):
            value = jnp.sum(diag[index] * wbuf[index : index + 1, :], axis=1, keepdims=True)
            acc = jnp.where(lane_k == half + index, value, acc)
        return mass16[...] * vector, acc

    def finish(turn, started, inputs):
        image, acc = started
        xbuf[0:half, :] = inputs
        found = coupled(0, acc).T
        image = image + dot(kept_hot, found) + found[half : half + pad, :]
        await_all(recv_b.at[turn], got.at[1 + 2 * turn], slots)
        return image + dot(land_hot[...], recv_b[turn, :, 0, :])

    for item in loads:
        item.wait()
    order_copy.wait()

    started = begin(0, vector)
    await_all(recv0, got.at[0], 1)

    def addressed(offset, count):
        size = n * count
        line = recv0[:, rb + offset : rb + offset + 1, :].reshape(n, 128)
        owner = jnp.floor((iota_f((size, n), 0) + 0.5) * (1.0 / count))
        spread = dot(hot(owner == iota_f((size, n), 1)), line + 1.0)
        row = iota_f((size, 128), 0)
        owner = jnp.floor((row + 0.5) * (1.0 / count))
        slot = row - owner * count
        lane = iota_f((size, 128), 1)
        mine = (lane == me_f * slots + slot) & (slot < slots) & (owner < n - 1)
        found = jnp.sum(jnp.where(mine, spread, 0.0), axis=1, keepdims=True) - 1.0
        return hot(found == lane)

    land_hot[...] = addressed(2, slots).T[0:pad, :]
    ask_hot[...] = addressed(1, lines)
    squares = jnp.sum(recv0[:, rb, :], axis=0, keepdims=True) + own_part
    beta = jnp.sqrt(pick(squares, 0))
    inputs = dot(first_hot, recv0[...].reshape(n * head, 128))
    image = finish(0, started, inputs)
    basis = [vector / beta]
    images = [image / beta]
    heads = []
    gram = {}

    for turn in range(1, ITERS):
        vector = images[-1]
        own_part = as_row(
            [total(vector * item) for item in basis]
            + [total(vector * item) for item in images]
        )
        wide_vector = jnp.concatenate([vector, jnp.zeros((128 - pad, 128), F32)], axis=0)
        blocks = dot(ask_hot[...], wide_vector)
        row = iota_f((lines_all, 128), 0)
        slot = row - jnp.floor((row + 0.5) * (1.0 / lines)) * lines
        send_a[turn - 1, :, 0, :] = jnp.where(slot == slots, own_part, blocks)
        broadcast(send_a.at[turn - 1], recv_a.at[turn - 1], 2 * turn, lines, True)
        started = begin(turn, vector)
        await_all(recv_a.at[turn - 1], got.at[2 * turn], lines)
        came = recv_a[turn - 1, :, 0, :]
        sums = jnp.sum(jnp.where(slot == slots, came, 0.0), axis=0, keepdims=True)
        sums = sums + own_part
        image = finish(turn, started, dot(fetch_hot, came))
        dots = [pick(sums, index) for index in range(turn)]
        for index in range(turn):
            gram[index, turn - 1] = pick(sums, turn + index)
        heads.append(dots[0])
        square = gram[turn - 1, turn - 1]
        left = square
        for value in dots:
            left = left - value * value
        scale = lax.rsqrt(jnp.maximum(left, square * 1e-6))
        for index in range(turn):
            vector = vector - dots[index] * basis[index]
            image = image - dots[index] * images[index]
        basis.append(vector * scale)
        images.append(image * scale)

    vector = images[-1]
    own_part = as_row(
        [total(vector * basis[0])] + [total(vector * item) for item in images]
    )
    send_f[0] = own_part
    broadcast(send_f, recv_f, 2 * ITERS, 1, False)
    await_all(recv_f, got.at[2 * ITERS], 1)
    sums = jnp.sum(recv_f[:, 0, :], axis=0, keepdims=True) + own_part
    heads.append(pick(sums, 0))
    for index in range(ITERS):
        gram[index, ITERS - 1] = pick(sums, 1 + index)

    factor = {}
    for i in range(ITERS):
        for j in range(i + 1):
            value = gram[j, i]
            for k in range(j):
                value = value - factor[i, k] * factor[j, k]
            factor[i, j] = jnp.sqrt(value) if i == j else value / factor[j, j]
    forward = []
    for i in range(ITERS):
        value = beta * heads[i]
        for k in range(i):
            value = value - factor[i, k] * forward[k]
        forward.append(value / factor[i, i])
    mixing = [None] * ITERS
    for i in reversed(range(ITERS)):
        value = forward[i]
        for k in range(i + 1, ITERS):
            value = value - factor[k, i] * mixing[k]
        mixing[i] = value / factor[i, i]
    update = mixing[0] * basis[0]
    for i in range(1, ITERS):
        update = update + mixing[i] * basis[i]
    out_ref[...] = update[0:rb, :]

    await_all(recv0, sent.at[0], 1)
    for turn in range(ITERS):
        await_all(send_b.at[turn], sent.at[1 + 2 * turn], slots)
    for turn in range(1, ITERS):
        await_all(send_a.at[turn - 1], sent.at[2 * turn], lines)
    await_all(recv_f, sent.at[2 * ITERS], 1)


def on_device(defect, mass, block_diag, coupling, tile_rows, tile_cols):
    rb, width = defect.shape
    tiles = tile_rows.shape[0]
    n = lax.axis_size("blk")
    slots = (tiles // 2 + n - 2) // (n - 1)
    pad = -(-rb // 8) * 8
    head = -(-(rb + 3) // 8) * 8
    vmem = pl.BlockSpec(memory_space=pltpu.VMEM)
    hbm = pl.BlockSpec(memory_space=pl.ANY)
    return pl.pallas_call(
        functools.partial(kernel, n, slots),
        out_shape=jax.ShapeDtypeStruct((rb, width), F32),
        in_specs=[vmem, vmem, hbm, hbm, vmem, vmem],
        out_specs=vmem,
        scratch_shapes=[
            pltpu.VMEM((tiles, width, width), F32),
            pltpu.VMEM((rb, width, width), F32),
            pltpu.VMEM((1, 128), jnp.int32),
            pltpu.SMEM((1, 128), jnp.int32),
            pltpu.VMEM((pad, width), F32),
            pltpu.VMEM((pad, width), F32),
            pltpu.VMEM((tiles, width), F32),
            pltpu.VMEM((n * (slots + 1), 128), F32),
            pltpu.VMEM((pad, n * slots), F32),
            pltpu.VMEM((1, head, width), F32),
            pltpu.VMEM((n, head, width), F32),
            pltpu.VMEM((ITERS - 1, n * (slots + 1), 1, width), F32),
            pltpu.VMEM((ITERS - 1, n * (slots + 1), 1, width), F32),
            pltpu.VMEM((ITERS, n * slots, 1, width), F32),
            pltpu.VMEM((ITERS, n * slots, 1, width), F32),
            pltpu.VMEM((1, 1, width), F32),
            pltpu.VMEM((n, 1, width), F32),
            pltpu.SemaphoreType.DMA((5,)),
            pltpu.SemaphoreType.DMA,
            pltpu.SemaphoreType.DMA((2 * ITERS + 1,)),
            pltpu.SemaphoreType.DMA((2 * ITERS + 1,)),
        ],
        compiler_params=pltpu.CompilerParams(collective_id=0, has_side_effects=True),
    )(
        defect,
        mass,
        block_diag,
        coupling,
        tile_rows.reshape(1, tiles),
        tile_cols.reshape(1, tiles),
    )


def solution(mesh):
    in_specs = (
        P("blk", None),
        P("blk", None),
        P("blk", None, None),
        P("blk", None, None),
        P("blk"),
        P("blk"),
    )
    return jax.shard_map(
        on_device, mesh=mesh, in_specs=in_specs, out_specs=P("blk", None), check_vma=False
    )
```

```python
import functools

import jax
import jax.numpy as jnp
from jax import lax
from jax.experimental import pallas as pl
from jax.experimental.pallas import tpu as pltpu
from jax.sharding import PartitionSpec as P

ITERS = 3
F32 = jnp.float32
MESH = pl.DeviceIdType.MESH


def iota(shape, axis):
    return lax.broadcasted_iota(jnp.int32, shape, axis)


def iota_f(shape, axis):
    return iota(shape, axis).astype(F32)


def dot(hot, value):
    hot = hot.astype(jnp.bfloat16)
    out = None
    for _ in range(3):
        piece = value.astype(jnp.bfloat16)
        value = value - piece.astype(F32)
        term = lax.dot_general(
            hot, piece, (((1,), (0,)), ((), ())), preferred_element_type=F32
        )
        out = term if out is None else out + term
    return out


def total(value):
    return jnp.sum(jnp.sum(value, axis=0, keepdims=True), axis=1, keepdims=True)


def as_row(items):
    lane = iota((1, 128), 1)
    row = jnp.zeros((1, 128), F32)
    for index, item in enumerate(items):
        row = jnp.where(lane == index, item, row)
    return row


def pick(row, index):
    lane = iota((1, 128), 1)
    return jnp.sum(jnp.where(lane == index, row, 0.0), axis=1, keepdims=True)


def kernel(
    n,
    slots,
    defect_ref,
    mass_ref,
    diag_hbm,
    coup_hbm,
    rows_ref,
    cols_ref,
    out_ref,
    coup,
    diag,
    order_v,
    order_s,
    mass16,
    wbuf,
    xbuf,
    ask_hot,
    land_hot,
    send0,
    recv0,
    send_a,
    recv_a,
    send_b,
    recv_b,
    send_f,
    recv_f,
    load_sems,
    order_sem,
    sent,
    got,
):
    me = lax.axis_index("blk")
    rb, width = defect_ref.shape
    tiles = rows_ref.shape[1]
    half = tiles // 2
    pad = wbuf.shape[0]
    head = send0.shape[1]
    parts = 4
    chunk = tiles // parts

    loads = [pltpu.make_async_copy(diag_hbm, diag, load_sems.at[parts])]
    for part in range(parts):
        span = pl.ds(part * chunk, chunk)
        loads.append(
            pltpu.make_async_copy(coup_hbm.at[span], coup.at[span], load_sems.at[part])
        )
    for item in loads:
        item.start()

    barrier = pltpu.get_barrier_semaphore()

    def peer(k):
        there = me + k
        return jnp.where(there >= n, there - n, there)

    for k in range(1, n):
        pl.semaphore_signal(barrier, inc=1, device_id=(peer(k),), device_id_type=MESH)

    rows = rows_ref[...]
    cols = cols_ref[...]
    low = me * rb
    pushes = (rows < low) | (rows >= low + rb)
    push_l = jnp.where(pushes, 1.0, 0.0)
    rem_l = jnp.where(pushes, rows, cols).astype(F32)
    loc_l = (jnp.where(pushes, cols, rows) - low).astype(F32)
    own_l = jnp.floor((rem_l + 0.5) * (1.0 / rb))
    far_l = rem_l - own_l * rb
    me_f = me.astype(F32)
    rel_l = own_l - me_f - 1.0
    rel_l = jnp.where(rel_l < 0.0, rel_l + n, rel_l)
    key_l = own_l + push_l * n
    square = (tiles, tiles)
    eye = iota(square, 0) == iota(square, 1)

    def to_s(value):
        return jnp.sum(jnp.where(eye, value, 0.0), axis=1, keepdims=True)

    earlier = iota(square, 0) < iota(square, 1)
    key_s = to_s(key_l)
    push_s = to_s(push_l)
    slot_l = jnp.sum(
        jnp.where((key_s == key_l) & earlier, 1.0, 0.0), axis=0, keepdims=True
    )
    pos_l = jnp.sum(
        jnp.where((push_s < push_l) | ((push_s == push_l) & earlier), 1.0, 0.0),
        axis=0,
        keepdims=True,
    )
    pos_s = to_s(pos_l)
    slot_s = to_s(slot_l)
    own_s = to_s(own_l)
    far_s = to_s(far_l)
    loc_s = to_s(loc_l)
    lines = slots + 1
    u_l = rel_l * lines + slot_l
    u_s = to_s(rel_l * slots + slot_l)
    wide = (tiles, 128)
    lane_w = iota_f(wide, 1)
    push_int = jnp.where(pushes, 1, 0)
    push_down = jnp.sum(jnp.where(eye, push_int, 0), axis=1, keepdims=True)
    place = jnp.sum(
        jnp.where(
            (push_down < push_int) | ((push_down == push_int) & earlier), 1, 0
        ),
        axis=0,
        keepdims=True,
    )
    place_down = jnp.sum(jnp.where(eye, place, 0), axis=1, keepdims=True)
    order_v[...] = jnp.sum(
        jnp.where(place_down == iota(wide, 1), iota(wide, 0), 0), axis=0, keepdims=True
    )
    order_copy = pltpu.make_async_copy(order_v, order_s, order_sem)
    order_copy.start()
    lane_1 = iota_f((1, 128), 1)
    push_u = jnp.sum(jnp.where(pos_s == lane_w + half, u_s, 0.0), axis=0, keepdims=True)
    push_u = jnp.where(lane_1 < half, push_u, -1.0)
    fetch_row = jnp.sum(jnp.where(pos_s == lane_w, loc_s, 0.0), axis=0, keepdims=True)
    fetch_row = jnp.where(lane_1 < half, fetch_row, -1.0)
    sorted_shape = (half, tiles)
    fetch_here = pos_l == iota_f(sorted_shape, 0)
    push_here = pos_l == iota_f(sorted_shape, 0) + half
    fetch_u = jnp.sum(jnp.where(fetch_here, u_l, 0.0), axis=1, keepdims=True)
    fetch_v = jnp.sum(
        jnp.where(fetch_here, rel_l * head + far_l, 0.0), axis=1, keepdims=True
    )
    push_col = jnp.sum(jnp.where(push_here, loc_l, 0.0), axis=1, keepdims=True)
    lane_key = own_s * slots + slot_s
    asks = jnp.sum(
        jnp.where((lane_key == lane_w) & (push_s < 0.5), far_s + 1.0, 0.0),
        axis=0,
        keepdims=True,
    ) - 1.0
    goals = jnp.sum(
        jnp.where((lane_key == lane_w) & (push_s > 0.5), far_s + 1.0, 0.0),
        axis=0,
        keepdims=True,
    ) - 1.0
    lines_all = n * lines
    slots_all = n * slots

    def hot(mask):
        return jnp.where(mask, 1.0, 0.0)

    wbuf[...] = jnp.zeros(wbuf.shape, F32)
    wbuf[0:rb, :] = -defect_ref[...]
    mass16[...] = jnp.zeros(mass16.shape, F32)
    mass16[0:rb, :] = mass_ref[...]
    vector = wbuf[...]
    send0[...] = jnp.zeros(send0.shape, F32)
    send0[0, 0:rb, :] = -defect_ref[...]
    own_part = as_row([total(vector * vector)])
    send0[0, rb : rb + 1, :] = own_part
    send0[0, rb + 1 : rb + 2, :] = asks
    send0[0, rb + 2 : rb + 3, :] = goals
    recv0[n - 1] = jnp.zeros(recv0.shape[1:], F32)
    for turn in range(ITERS):
        recv_b[turn, slots_all - slots : slots_all] = jnp.zeros((slots, 1, 128), F32)
    for turn in range(ITERS - 1):
        recv_a[turn, lines_all - lines : lines_all] = jnp.zeros((lines, 1, 128), F32)
    recv_f[n - 1] = jnp.zeros((1, 128), F32)

    pl.semaphore_wait(barrier, n - 1)

    def broadcast(source, target, index, count, spread):
        for k in range(1, n):
            start = (n - 1 - k) * count
            pltpu.make_async_remote_copy(
                src_ref=source.at[pl.ds((k - 1) * count, count)] if spread else source,
                dst_ref=target.at[pl.ds(start, count)],
                send_sem=sent.at[index],
                recv_sem=got.at[index],
                device_id=(peer(k),),
                device_id_type=MESH,
            ).start()

    def await_all(target, sem, count):
        view = target.at[pl.ds(0, (n - 1) * count)]
        pltpu.make_async_copy(view, view, sem).wait()

    broadcast(send0, recv0, 0, 1, False)

    spread_hot = hot(iota_f((slots_all, 128), 0) == push_u)
    fetch_hot = hot(iota_f((half, lines_all), 1) == fetch_u)
    first_hot = hot(iota_f((half, n * head), 1) == fetch_v)
    input_hot = hot(iota_f((half, pad), 1) == push_col)
    kept_hot = hot(iota_f((pad, 128), 0) == fetch_row)

    lane_k = iota((width, 128), 1)

    def matvec(acc, tile, index):
        row = xbuf[index : index + 1, :]
        value = jnp.sum(tile * row, axis=1, keepdims=True)
        return jnp.where(lane_k == index, value, acc)

    def coupled(base, acc):
        for index in range(half):
            tile = jnp.clip(order_s[0, base + index], 0, 2 * half - 1)
            acc = matvec(acc, coup[tile], index)
        return acc

    empty = jnp.zeros((width, 128), F32)

    def begin(turn, vector):
        xbuf[0:half, :] = dot(input_hot, vector)
        found = coupled(half, empty).T
        send_b[turn, :, 0, :] = dot(spread_hot, found)
        broadcast(send_b.at[turn], recv_b.at[turn], 1 + 2 * turn, slots, True)
        wbuf[...] = vector
        acc = empty
        for index in range(rb):
            value = jnp.sum(diag[index] * wbuf[index : index + 1, :], axis=1, keepdims=True)
            acc = jnp.where(lane_k == half + index, value, acc)
        return mass16[...] * vector, acc

    def finish(turn, started, inputs):
        image, acc = started
        xbuf[0:half, :] = inputs
        found = coupled(0, acc).T
        image = image + dot(kept_hot, found) + found[half : half + pad, :]
        await_all(recv_b.at[turn], got.at[1 + 2 * turn], slots)
        return image + dot(land_hot[...], recv_b[turn, :, 0, :])

    for item in loads:
        item.wait()
    order_copy.wait()

    started = begin(0, vector)
    await_all(recv0, got.at[0], 1)

    def addressed(offset, count):
        size = n * count
        line = recv0[:, rb + offset : rb + offset + 1, :].reshape(n, 128)
        owner = jnp.floor((iota_f((size, n), 0) + 0.5) * (1.0 / count))
        spread = dot(hot(owner == iota_f((size, n), 1)), line + 1.0)
        row = iota_f((size, 128), 0)
        owner = jnp.floor((row + 0.5) * (1.0 / count))
        slot = row - owner * count
        lane = iota_f((size, 128), 1)
        mine = (lane == me_f * slots + slot) & (slot < slots) & (owner < n - 1)
        found = jnp.sum(jnp.where(mine, spread, 0.0), axis=1, keepdims=True) - 1.0
        return hot(found == lane)

    land_hot[...] = addressed(2, slots).T[0:pad, :]
    ask_hot[...] = addressed(1, lines)
    squares = jnp.sum(recv0[:, rb, :], axis=0, keepdims=True) + own_part
    beta = jnp.sqrt(pick(squares, 0))
    inputs = dot(first_hot, recv0[...].reshape(n * head, 128))
    image = finish(0, started, inputs)
    basis = [vector / beta]
    images = [image / beta]
    heads = []
    gram = {}

    for turn in range(1, ITERS):
        vector = images[-1]
        own_part = as_row(
            [total(vector * item) for item in basis]
            + [total(vector * item) for item in images]
        )
        wide_vector = jnp.concatenate([vector, jnp.zeros((128 - pad, 128), F32)], axis=0)
        blocks = dot(ask_hot[...], wide_vector)
        row = iota_f((lines_all, 128), 0)
        slot = row - jnp.floor((row + 0.5) * (1.0 / lines)) * lines
        send_a[turn - 1, :, 0, :] = jnp.where(slot == slots, own_part, blocks)
        broadcast(send_a.at[turn - 1], recv_a.at[turn - 1], 2 * turn, lines, True)
        started = begin(turn, vector)
        await_all(recv_a.at[turn - 1], got.at[2 * turn], lines)
        came = recv_a[turn - 1, :, 0, :]
        sums = jnp.sum(jnp.where(slot == slots, came, 0.0), axis=0, keepdims=True)
        sums = sums + own_part
        image = finish(turn, started, dot(fetch_hot, came))
        dots = [pick(sums, index) for index in range(turn)]
        for index in range(turn):
            gram[index, turn - 1] = pick(sums, turn + index)
        heads.append(dots[0])
        square = gram[turn - 1, turn - 1]
        left = square
        for value in dots:
            left = left - value * value
        scale = lax.rsqrt(jnp.maximum(left, square * 1e-6))
        for index in range(turn):
            vector = vector - dots[index] * basis[index]
            image = image - dots[index] * images[index]
        basis.append(vector * scale)
        images.append(image * scale)

    vector = images[-1]
    own_part = as_row(
        [total(vector * basis[0])] + [total(vector * item) for item in images]
    )
    send_f[0] = own_part
    broadcast(send_f, recv_f, 2 * ITERS, 1, False)
    await_all(recv_f, got.at[2 * ITERS], 1)
    sums = jnp.sum(recv_f[:, 0, :], axis=0, keepdims=True) + own_part
    heads.append(pick(sums, 0))
    for index in range(ITERS):
        gram[index, ITERS - 1] = pick(sums, 1 + index)

    factor = {}
    for i in range(ITERS):
        for j in range(i + 1):
            value = gram[j, i]
            for k in range(j):
                value = value - factor[i, k] * factor[j, k]
            factor[i, j] = jnp.sqrt(value) if i == j else value / factor[j, j]
    forward = []
    for i in range(ITERS):
        value = beta * heads[i]
        for k in range(i):
            value = value - factor[i, k] * forward[k]
        forward.append(value / factor[i, i])
    mixing = [None] * ITERS
    for i in reversed(range(ITERS)):
        value = forward[i]
        for k in range(i + 1, ITERS):
            value = value - factor[k, i] * mixing[k]
        mixing[i] = value / factor[i, i]
    update = mixing[0] * basis[0]
    for i in range(1, ITERS):
        update = update + mixing[i] * basis[i]
    out_ref[...] = update[0:rb, :]

    await_all(recv0, sent.at[0], 1)
    for turn in range(ITERS):
        await_all(send_b.at[turn], sent.at[1 + 2 * turn], slots)
    for turn in range(1, ITERS):
        await_all(send_a.at[turn - 1], sent.at[2 * turn], lines)
    await_all(recv_f, sent.at[2 * ITERS], 1)


def on_device(defect, mass, block_diag, coupling, tile_rows, tile_cols):
    rb, width = defect.shape
    tiles = tile_rows.shape[0]
    n = lax.axis_size("blk")
    slots = (tiles // 2 + n - 2) // (n - 1)
    pad = -(-rb // 8) * 8
    head = -(-(rb + 3) // 8) * 8
    vmem = pl.BlockSpec(memory_space=pltpu.VMEM)
    hbm = pl.BlockSpec(memory_space=pl.ANY)
    return pl.pallas_call(
        functools.partial(kernel, n, slots),
        out_shape=jax.ShapeDtypeStruct((rb, width), F32),
        in_specs=[vmem, vmem, hbm, hbm, vmem, vmem],
        out_specs=vmem,
        scratch_shapes=[
            pltpu.VMEM((tiles, width, width), F32),
            pltpu.VMEM((rb, width, width), F32),
            pltpu.VMEM((1, 128), jnp.int32),
            pltpu.SMEM((1, 128), jnp.int32),
            pltpu.VMEM((pad, width), F32),
            pltpu.VMEM((pad, width), F32),
            pltpu.VMEM((tiles, width), F32),
            pltpu.VMEM((n * (slots + 1), 128), F32),
            pltpu.VMEM((pad, n * slots), F32),
            pltpu.VMEM((1, head, width), F32),
            pltpu.VMEM((n, head, width), F32),
            pltpu.VMEM((ITERS - 1, n * (slots + 1), 1, width), F32),
            pltpu.VMEM((ITERS - 1, n * (slots + 1), 1, width), F32),
            pltpu.VMEM((ITERS, n * slots, 1, width), F32),
            pltpu.VMEM((ITERS, n * slots, 1, width), F32),
            pltpu.VMEM((1, 1, width), F32),
            pltpu.VMEM((n, 1, width), F32),
            pltpu.SemaphoreType.DMA((5,)),
            pltpu.SemaphoreType.DMA,
            pltpu.SemaphoreType.DMA((2 * ITERS + 1,)),
            pltpu.SemaphoreType.DMA((2 * ITERS + 1,)),
        ],
        compiler_params=pltpu.CompilerParams(collective_id=0, has_side_effects=True),
    )(
        defect,
        mass,
        block_diag,
        coupling,
        tile_rows.reshape(1, tiles),
        tile_cols.reshape(1, tiles),
    )


def solution(mesh):
    in_specs = (
        P("blk", None),
        P("blk", None),
        P("blk", None, None),
        P("blk", None, None),
        P("blk"),
        P("blk"),
    )
    return jax.shard_map(
        on_device, mesh=mesh, in_specs=in_specs, out_specs=P("blk", None), check_vma=False
    )
```
